32 devices in a mesh: zero: 4 (over y, x), cols: 4 (over z), copy: 2 (over core).
Axes of the slice: x: 2, y: 2, z: 4, core: 2. Of those that a mesh axis runs over, the one named last changes fastest.
Arguments:
- weight_query: bfloat16 [8192, 4096], P(('copy', 'zero'), 'cols'), parts along dimension 0, may hold values from -0.125 to 0.125
- low_query: bfloat16 [8192, 32], P(('copy', 'zero')), parts along dimension 0, may hold values from -0.09375 to 0.09375
- high_query: bfloat16 [64, 4096], P('copy', 'cols'), parts along dimension 0, may hold values from -1 to 1
- weight_key: bfloat16 [8192, 4096], P(('copy', 'zero'), 'cols'), parts along dimension 0, may hold values from -0.125 to 0.125
- low_key: bfloat16 [8192, 32], P(('copy', 'zero')), parts along dimension 0, may hold values from -0.09375 to 0.09375
- high_key: bfloat16 [64, 4096], P('copy', 'cols'), parts along dimension 0, may hold values from -1 to 1
- weight_value: bfloat16 [8192, 4096], P(('copy', 'zero'), 'cols'), parts along dimension 0, may hold values from -0.125 to 0.125
- low_value: bfloat16 [8192, 32], P(('copy', 'zero')), parts along dimension 0, may hold values from -0.09375 to 0.09375
- high_value: bfloat16 [64, 4096], P('copy', 'cols'), parts along dimension 0, may hold values from -1 to 1
- norm_train: float32 [8192], P(('copy', 'zero', 'cols')), parts along dimension 0, may hold values from 0.25 to 1.75
- norm_step: float32 [8192], P(('copy', 'zero', 'cols')), parts along dimension 0, may hold values from -0.3 to 0.3
Outputs:
- final_query: bfloat16 [8192, 4096], P('copy', 'cols'), parts along dimension 0
- final_key: bfloat16 [8192, 4096], P('copy', 'cols'), parts along dimension 0
- final_value: bfloat16 [8192, 4096], P('copy', 'cols'), parts along dimension 0
- scale_query: float32 [8192], P(('copy', 'cols')), parts along dimension 0
- scale_key: float32 [8192], P(('copy', 'cols')), parts along dimension 0
- scale_value: float32 [8192], P(('copy', 'cols')), parts along dimension 0
- serve_norm: bfloat16 [8192], P('copy'), parts along dimension 0
The draws below stay inside these ranges and needn't reach their ends.
There are 2 independent parts, one for each index of `copy`. The reference program is written for one: setup_inputs(seed, part) draws one part's arguments, and reference() takes and returns one part's arrays. A program takes and returns all parts, laid end to end along the dimension named above; each array names one. Nothing has to cross between parts.
All inputs are finite; a program needn't handle non-finite values.
Results may differ from the reference program's by a relative error of at most 0.00075.
Values may be sent and summed in bfloat16 or wider, within the bound.
No kernel may reach another device: no remote copies, remote signals or barrier semaphores. Data moves between devices by JAX's collectives and lax.ppermute only.
A program may use at most 128 MiB of HBM per device.

```python
import jax
import jax.numpy as jnp
from jax import lax

D_MODEL = 4096
Q_DIM = 4096
KV_DIM = 4096
RANK = 32


def with_spikes(entries, key, source, target, parts, factor):
    owner, partner = [(jnp.arange(entries.shape[dim]) // (entries.shape[dim] // parts)).reshape([-1 if axis == dim else 1 for axis in range(entries.ndim)]) for dim in (source, target)]
    chosen = jax.random.permutation(key, parts)[partner]
    strong = (owner == chosen) | (owner == (partner + parts // 2) % parts)
    return jnp.where(strong, factor * entries, entries)


def level_of(key, shape, shards, low, top_value):
    def one(dim, blocks):
        heights = jax.random.uniform(jax.random.fold_in(jax.random.fold_in(key, 6), dim), (blocks,), jnp.float32, low / len(shards), top_value / len(shards))
        return jnp.repeat(jnp.exp(heights), shape[dim] // blocks).reshape((-1,) + (1,) * (len(shape) - dim - 1))

    loudness = one(*shards[0])
    for cut in shards[1:]:
        loudness = loudness * one(*cut)
    return loudness


def centred(rng, dims, scale, limit, cuts=(), dtype=jnp.bfloat16):
    values = scale * jax.random.normal(rng, dims, jnp.float32)
    if cuts:
        values = values * level_of(rng, dims, cuts, -0.22, 0.18)
    return jnp.clip(values, -limit, limit).astype(dtype)


def noise_with(stream_key, extent, scale, reach, split, heavy, held_as=jnp.bfloat16):
    entries = scale * jax.random.normal(stream_key, extent, jnp.float32)
    if split:
        entries = entries * level_of(stream_key, extent, split, -0.22, 0.18)
    return jnp.clip(with_spikes(entries, jax.random.fold_in(stream_key, 3), *heavy), -reach, reach).astype(held_as)


def setup_inputs(seed: int = 0, part: int = 0) -> dict:
    key_list = jax.random.split(jax.random.key(seed), 12)
    part_keys = jax.random.split(jax.random.fold_in(key_list[11], part), 12)
    weight_query = noise_with(part_keys[0], (D_MODEL, Q_DIM), D_MODEL ** -0.5, 0.125, ((0, 4), (1, 4)), (0, 1, 4, 2.0))
    low_query = centred(part_keys[1], (D_MODEL, RANK), D_MODEL ** -0.5, 0.09375, ((0, 4),))
    high_query = centred(part_keys[2], (RANK, Q_DIM), RANK ** -0.5, 1.0, ((1, 4),))
    weight_key = noise_with(part_keys[3], (D_MODEL, KV_DIM), D_MODEL ** -0.5, 0.125, ((0, 4), (1, 4)), (0, 1, 4, 2.0))
    low_key = centred(part_keys[4], (D_MODEL, RANK), D_MODEL ** -0.5, 0.09375, ((0, 4),))
    high_key = centred(part_keys[5], (RANK, KV_DIM), RANK ** -0.5, 1.0, ((1, 4),))
    weight_value = noise_with(part_keys[6], (D_MODEL, KV_DIM), D_MODEL ** -0.5, 0.125, ((0, 4), (1, 4)), (0, 1, 4, 2.0))
    low_value = centred(part_keys[7], (D_MODEL, RANK), D_MODEL ** -0.5, 0.09375, ((0, 4),))
    high_value = centred(part_keys[8], (RANK, KV_DIM), RANK ** -0.5, 1.0, ((1, 4),))
    norm_train = jnp.clip(1.0 + 0.15 * jax.random.normal(part_keys[9], (D_MODEL,), jnp.float32), 0.25, 1.75)
    norm_step = jnp.clip(jax.random.uniform(part_keys[10], (D_MODEL,), jnp.float32, -0.3, 0.3) * level_of(part_keys[10], (D_MODEL,), ((0, 16),), -0.4, 0.0), -0.3, 0.3)
    return {"weight_query": weight_query, "low_query": low_query, "high_query": high_query, "weight_key": weight_key, "low_key": low_key, "high_key": high_key, "weight_value": weight_value, "low_value": low_value, "high_value": high_value, "norm_train": norm_train, "norm_step": norm_step}


mix_rate = 2.0

def reference(weight_query, low_query, high_query, weight_key, low_key, high_key, weight_value, low_value, high_value, norm_train, norm_step):
    result_query = weight_query.astype(jnp.float32) + mix_rate * jnp.dot(low_query, high_query, preferred_element_type=jnp.float32)
    result_key = weight_key.astype(jnp.float32) + mix_rate * jnp.dot(low_key, high_key, preferred_element_type=jnp.float32)
    result_value = weight_value.astype(jnp.float32) + mix_rate * jnp.dot(low_value, high_value, preferred_element_type=jnp.float32)
    scale_query = jnp.sqrt(lax.optimization_barrier(jnp.sum(result_query * result_query, axis=0)))
    final_query = (result_query / scale_query).astype(jnp.bfloat16)
    scale_key = jnp.sqrt(lax.optimization_barrier(jnp.sum(result_key * result_key, axis=0)))
    final_key = (result_key / scale_key).astype(jnp.bfloat16)
    scale_value = jnp.sqrt(lax.optimization_barrier(jnp.sum(result_value * result_value, axis=0)))
    final_value = (result_value / scale_value).astype(jnp.bfloat16)
    serve_norm = (norm_train + norm_step).astype(jnp.bfloat16)
    return (final_query, final_key, final_value, scale_query, scale_key, scale_value, serve_norm)
```

```python
import math

import jax
import jax.numpy as jnp
from jax import lax
from jax.sharding import PartitionSpec as P

mix_rate = 2.0


def grid_of(total):
    across = next(n for n in range(math.isqrt(total), 0, -1) if total % n == 0)
    return total // across, across


def merged(weight, low, high):
    return weight.astype(jnp.float32) + mix_rate * jnp.dot(
        low, high, preferred_element_type=jnp.float32
    )


def program(zero, cols):
    down, across = grid_of(zero)

    def moved(value, dy, dx, name):
        pairs = [
            (y * across + x, (y + dy) % down * across + (x + dx) % across)
            for y in range(down)
            for x in range(across)
        ]
        with jax.named_scope(name):
            return lax.ppermute(value, "zero", pairs)

    def body(
        weight_query,
        low_query,
        high_query,
        weight_key,
        low_key,
        high_key,
        weight_value,
        low_value,
        high_value,
        norm_train,
        norm_step,
    ):
        rows, width = weight_query.shape
        half = rows // 2
        me = lax.axis_index("zero")
        mine_y, mine_x = me // across, me % across

        def owner(dy, dx):
            return (mine_y - dy) % down * across + (mine_x - dx) % across

        def blank():
            return jnp.zeros((zero * 2, half, width), jnp.bfloat16)

        def put(out, piece, dy, dx, part):
            pieces = piece.reshape(-1, half, width)
            return lax.dynamic_update_slice(out, pieces, (owner(dy, dx) * 2 + part, 0, 0))

        peers = [(0, dx) for dx in range(1, across)] + [(dy, 0) for dy in range(1, down)]
        others = [
            (dy, dx) for dy in range(down) for dx in range(across) if (dy, dx) != (0, 0)
        ]

        top, bottom = weight_query[:half], weight_query[half:]
        raw = {p: [moved(top, *p, f"raw_top_{p[0]}{p[1]}")] for p in peers}
        low_of = {p: moved(low_query, *p, f"raw_low_{p[0]}{p[1]}") for p in peers}

        result = [
            merged(weight_query, low_query, high_query),
            merged(weight_key, low_key, high_key),
            merged(weight_value, low_value, high_value),
        ]
        own = jnp.stack([jnp.sum(r * r, axis=0) for r in result])
        sums = {(0, 0): own}
        for p in others:
            sums[p] = moved(own, *p, f"sums_{p[0]}{p[1]}")
        for p in peers:
            raw[p].append(moved(bottom, *p, f"raw_bottom_{p[0]}{p[1]}"))
        table = jnp.zeros((zero,) + own.shape, jnp.float32)
        for p, value in sums.items():
            table = lax.dynamic_update_slice(table, value[None], (owner(*p), 0, 0))
        scale = jnp.sqrt(jnp.sum(table, axis=0))

        narrow = [(result[i] / scale[i]).astype(jnp.bfloat16) for i in range(3)]

        got = [{}, {}, {}]
        for i in (1, 2):
            for p in peers:
                block = moved(narrow[i], *p, f"own{i}_{p[0]}{p[1]}")
                got[i][p] = [block[:half], block[half:]]
        for p in peers:
            got[0][p] = [
                (
                    merged(piece, low_of[p][part * half : (part + 1) * half], high_query)
                    / scale[0]
                ).astype(jnp.bfloat16)
                for part, piece in enumerate(raw[p])
            ]

        finals = []
        for i in range(3):
            out = put(blank(), narrow[i], 0, 0, 0)
            for p in peers:
                for part in (0, 1):
                    out = put(out, got[i][p][part], *p, part)
            for dy in range(1, down):
                for dx in range(1, across):
                    upper = moved(got[i][(0, dx)][0], dy, 0, f"fwd{i}_{dy}{dx}_top")
                    lower = moved(got[i][(dy, 0)][1], 0, dx, f"fwd{i}_{dy}{dx}_bottom")
                    out = put(out, upper, dy, dx, 0)
                    out = put(out, lower, dy, dx, 1)
            finals.append(out.reshape(zero * rows, width))

        gain = (norm_train + norm_step).astype(jnp.bfloat16)
        column = lax.axis_index("cols")
        line = jnp.zeros((cols, gain.shape[0]), jnp.bfloat16)
        line = lax.dynamic_update_slice(line, gain[None], (column, 0))
        for shift in range(1, cols):
            with jax.named_scope(f"gain_cols_{shift}"):
                value = lax.ppermute(
                    gain, "cols", [(c, (c + shift) % cols) for c in range(cols)]
                )
            line = lax.dynamic_update_slice(line, value[None], ((column - shift) % cols, 0))
        plane = jnp.zeros((zero,) + line.shape, jnp.bfloat16)
        plane = lax.dynamic_update_slice(plane, line[None], (me, 0, 0))
        for p in others:
            value = moved(line, *p, f"gain_zero_{p[0]}{p[1]}")
            plane = lax.dynamic_update_slice(plane, value[None], (owner(*p), 0, 0))
        serve_norm = plane.reshape(-1)
        return (*finals, scale[0], scale[1], scale[2], serve_norm)

    return body


def solution(mesh):
    placed = (
        P(("copy", "zero"), "cols"),
        P(("copy", "zero"), None),
        P("copy", "cols"),
    ) * 3 + (P(("copy", "zero", "cols")),) * 2
    return jax.shard_map(
        program(mesh.shape["zero"], mesh.shape["cols"]),
        mesh=mesh,
        in_specs=placed,
        out_specs=(P("copy", "cols"),) * 3 + (P(("copy", "cols")),) * 3 + (P("copy"),),
        check_vma=False,
    )
```
